32 devices in a mesh: gx: 16 (over z, y, core), gy: 2 (over x).
Axes of the slice: x: 2, y: 2, z: 4, core: 2. Of those that a mesh axis runs over, the one named last changes fastest.
Arguments:
- right_side: float32 [16, 2, 512, 256], P('gx', 'gy'), may hold values from -8 to 8, as said below
- coords: float32 [16, 2, 2, 512], P('gx', 'gy'), may hold values from 0 to 1
- noise: float32 [16, 2, 512], P('gx', 'gy'), may hold values from 0.25 to 1
- intersect: int32 [16, 2, 128], P('gx', 'gy'), may hold values from 0 to 4607, as said below
Outputs:
- solution: float32 [16, 2, 512, 256], P('gx', 'gy')
- residual: float32 [16, 2, 512, 256], P('gx', 'gy')
The draws below stay inside these ranges and needn't reach their ends.
Inputs may be any that keep to these rules, and one draw needn't show every extreme that they name: `right_side`: right-hand sides of order one. `intersect`: each subdomain's list holds 128 distinct indices in increasing order; none names the subdomain itself (block number 4) or a subdomain beyond the first or last one along the second dimension.
All inputs are finite; a program needn't handle non-finite values.
Results may differ from the reference program's by a relative error of at most 0.0003.
Values sent between devices are 32-bit elements; how exact they have to be, the bound alone decides.
A program may use at most 128 MiB of HBM per device.

```python
import math
import jax
import jax.numpy as jnp
from jax import lax

P_SIZE = 512
OV = 128
R = 256
ITERS = 3
CELLS_X = 16
CELLS_Y = 2


def draw_right_side(key, part):
    full_shape = (CELLS_X, CELLS_Y, P_SIZE, R)
    normal_vals = jax.random.normal(key, full_shape, jnp.float32)
    return jnp.clip(normal_vals, -6.0, 6.0)


def draw_intersect(key, part):
    slot_count = 9 * P_SIZE

    def per_cell(cell_id):
        cell_key = jax.random.fold_in(key, cell_id + 7)
        column_id = cell_id % CELLS_Y
        slot_ids = jnp.arange(slot_count, dtype=jnp.int32)
        block_col = slot_ids // P_SIZE % 3
        banned = (slot_ids // P_SIZE == 4) | (block_col == 0) & (column_id == 0) | (block_col == 2) & (column_id == CELLS_Y - 1)
        scores = jax.random.randint(cell_key, (slot_count,), 0, 131072, dtype=jnp.int32) * slot_count + slot_ids
        scores = jnp.where(banned, 1073741824 + slot_ids, scores)
        ranking = jnp.argsort(scores, stable=True)
        return jnp.sort(ranking[:OV]).astype(jnp.int32)
    chosen = jax.vmap(per_cell)(jnp.arange(CELLS_X * CELLS_Y, dtype=jnp.int32))
    return chosen.reshape(CELLS_X, CELLS_Y, OV)


def steps_of(stream_key, shape, shards, smallest, high):
    def one(position, parts):
        heights = jax.random.uniform(jax.random.fold_in(jax.random.fold_in(stream_key, 6), position), (parts,), jnp.float32, smallest / len(shards), high / len(shards))
        return jnp.repeat(jnp.exp(heights), shape[position] // parts).reshape((-1,) + (1,) * (len(shape) - position - 1))

    level = one(*shards[0])
    for cut in shards[1:]:
        level = level * one(*cut)
    return level


def setup_inputs(seed: int = 0) -> dict:
    keys = jax.random.split(jax.random.key(seed), 5)
    right_side = draw_right_side(jax.random.fold_in(keys[4], 71), 0)
    coords = jnp.clip(1.0 * jax.random.uniform(keys[1], (CELLS_X, CELLS_Y, 2, P_SIZE), jnp.float32) ** steps_of(keys[1], (CELLS_X, CELLS_Y, 2, P_SIZE), ((0, 16), (1, 2)), -0.2, 0.2), 0.0, 1.0)
    noise = jnp.clip(jnp.exp(math.log(1.0) - 1.3862944 * jax.random.uniform(keys[2], (CELLS_X, CELLS_Y, P_SIZE), jnp.float32) ** steps_of(keys[2], (CELLS_X, CELLS_Y, P_SIZE), ((0, 16), (1, 2)), -0.2, 0.2)), 0.25, 1.0)
    intersect = draw_intersect(jax.random.fold_in(keys[4], 71), 0)
    return {"right_side": right_side, "coords": coords, "noise": noise, "intersect": intersect}


RANGE_LEN = 0.25
ROOT_THREE = math.sqrt(3.0)
HIGH = lax.Precision.HIGHEST

def kernel_block(rows_pos, cols_pos):
    delta_x = rows_pos[0][:, None] - cols_pos[0][None, :]
    delta_y = rows_pos[1][:, None] - cols_pos[1][None, :]
    distance = jnp.sqrt(delta_x * delta_x + delta_y * delta_y)
    scaled = ROOT_THREE / RANGE_LEN * distance
    clipped = jnp.minimum(distance, 1.0)
    taper_val = jnp.square(jnp.square(1.0 - clipped)) * (4.0 * clipped + 1.0)
    return (1.0 + scaled) * jnp.exp(-scaled) * taper_val

def reference(right_side, coords, noise, intersect):
    cells_x, cells_y, points, rhs_count = right_side.shape
    intersect_len = intersect.shape[2]
    cell_count = cells_x * cells_y
    ext_len = points + intersect_len

    def neighbour(values, cell_row, cell_col, shift_x, shift_y):
        near_row = (cell_row + shift_x) % cells_x
        near_col = cell_col + shift_y
        inside = (near_col >= 0) & (near_col < cells_y)
        fetched = values[near_row, jnp.clip(near_col, 0, cells_y - 1)]
        return jnp.where(inside, fetched, jnp.zeros_like(fetched))

    def operate(vector):

        def per_cell(cell_id):
            cell_row = cell_id // cells_y
            cell_col = cell_id % cells_y
            own_pos = coords[cell_row, cell_col]
            accumulated = noise[cell_row, cell_col][:, None] * vector[cell_row, cell_col]
            for shift_x in (-1, 0, 1):
                for shift_y in (-1, 0, 1):
                    near_info = neighbour(coords, cell_row, cell_col, shift_x, shift_y)
                    near_pos = jnp.stack([near_info[0] + float(shift_x), near_info[1] + float(shift_y)])
                    near_vec = neighbour(vector, cell_row, cell_col, shift_x, shift_y)
                    accumulated = accumulated + jnp.dot(kernel_block(own_pos, near_pos).astype(jnp.float32), near_vec.astype(jnp.float32), precision=HIGH, preferred_element_type=jnp.float32)
            return accumulated
        result = lax.map(per_cell, jnp.arange(cell_count, dtype=jnp.int32))
        return result.reshape(cells_x, cells_y, points, rhs_count)

    def setup_cell(cell_id):
        cell_row = cell_id // cells_y
        cell_col = cell_id % cells_y
        intersect_ids = intersect[cell_row, cell_col]
        block_id = intersect_ids // points
        row_in = intersect_ids % points
        row_of = block_id // 3
        col_of = block_id % 3
        near_row = ((cell_row + row_of - 1) % cells_x).astype(jnp.int32)
        near_col = (cell_col + col_of - 1).astype(jnp.int32)
        pos_x = coords[near_row, near_col, 0, row_in]
        pos_y = coords[near_row, near_col, 1, row_in]
        ov_pos = jnp.stack([pos_x + (row_of - 1).astype(jnp.float32), pos_y + (col_of - 1).astype(jnp.float32)])
        ext_pos = jnp.concatenate([coords[cell_row, cell_col], ov_pos], axis=1)
        ext_noise = jnp.concatenate([noise[cell_row, cell_col], noise[near_row, near_col, row_in]])
        local_matrix = kernel_block(ext_pos, ext_pos) + jnp.diag(ext_noise)
        factor = jnp.linalg.cholesky(local_matrix)
        inv_factor = lax.linalg.triangular_solve(factor, jnp.eye(ext_len, dtype=jnp.float32), left_side=True, lower=True)
        inverse = jnp.dot(inv_factor.T.astype(jnp.float32), inv_factor.astype(jnp.float32), precision=HIGH, preferred_element_type=jnp.float32)
        global_ids = ((near_row * cells_y + near_col) * points + row_in).astype(jnp.int32)
        return (inverse, global_ids)
    inverses, global_ids = lax.map(setup_cell, jnp.arange(cell_count, dtype=jnp.int32))

    def precondition(residue):
        flat_res = residue.reshape(cell_count * points, rhs_count)
        extended = jnp.concatenate([residue.reshape(cell_count, points, rhs_count), flat_res[global_ids]], axis=1)
        solved = jnp.einsum('cij,cjr->cir', inverses, extended, precision=HIGH)
        result = solved[:, :points].reshape(cell_count * points, rhs_count)
        result = result.at[global_ids.reshape(-1)].add(solved[:, points:].reshape(-1, rhs_count))
        return result.reshape(cells_x, cells_y, points, rhs_count)

    def column_sum(first, second):
        return lax.optimization_barrier(jnp.sum(first * second, axis=(0, 1, 2)))
    solution = jnp.zeros_like(right_side)
    residual = right_side
    precond = precondition(residual)
    direction = precond
    inner_now = column_sum(residual, precond)
    for iteration in range(ITERS):
        image_vec = operate(direction)
        step_size = inner_now / column_sum(direction, image_vec)
        solution = solution + step_size * direction
        residual = residual - step_size * image_vec
        if iteration + 1 < ITERS:
            precond = precondition(residual)
            inner_next = column_sum(residual, precond)
            direction = precond + inner_next / inner_now * direction
            inner_now = inner_next
    return (solution, residual)
```

```python
import functools
import math

import jax
import jax.numpy as jnp
from jax import lax
from jax.experimental import pallas as pl
from jax.experimental.pallas import tpu as pltpu
from jax.sharding import PartitionSpec as P

ITERS = 3


RANGE_LEN = 0.25
ROOT_THREE = math.sqrt(3.0)
HIGH = lax.Precision.HIGHEST


def shifted(value, axis, by):
    count = lax.axis_size(axis)
    return lax.ppermute(value, axis, [(i, (i + by) % count) for i in range(count)])


def passed_along(block, axis, distance):
    devices = range(lax.axis_size(axis))
    route = [(i - distance, i) for i in devices if i - distance in devices]
    return lax.ppermute(block, axis, route)


def kernel_block(rows_pos, cols_pos):
    delta_x = rows_pos[0][:, None] - cols_pos[0][None, :]
    delta_y = rows_pos[1][:, None] - cols_pos[1][None, :]
    distance = jnp.sqrt(delta_x * delta_x + delta_y * delta_y)
    scaled = ROOT_THREE / RANGE_LEN * distance
    clipped = jnp.minimum(distance, 1.0)
    taper_val = jnp.square(jnp.square(1.0 - clipped)) * (4.0 * clipped + 1.0)
    return (1.0 + scaled) * jnp.exp(-scaled) * taper_val


def window_values(values):
    beside = {}
    for step_by in (1, -1):
        beside[step_by] = shifted(values, "gx", step_by)
    column = jnp.stack([beside[1], values, beside[-1]])
    across = {}
    for step_by in (1, -1):
        across[step_by] = passed_along(column, "gy", step_by)
    return [across[1], column, across[-1]]


def window_index(values):
    beside = {}
    for step_by in (1, -1):
        beside[step_by] = shifted(values, "gx", step_by)
    column = jnp.stack([beside[1], values, beside[-1]])
    across = {}
    for step_by in (1, -1):
        across[step_by] = passed_along(column, "gy", step_by)
    return [across[1], column, across[-1]]


MESH = pl.DeviceIdType.MESH
NOISE_MIN = 0.25
VMEM = pl.BlockSpec(memory_space=pltpu.VMEM)


def split(value):
    top = value.astype(jnp.bfloat16)
    return top, (value - top.astype(jnp.float32)).astype(jnp.bfloat16)


def dot3(left, right):
    left_top, left_low = split(left)
    right_top, right_low = split(right)
    return jnp.dot(
        jnp.concatenate([left_top, left_top, left_low], axis=1),
        jnp.concatenate([right_top, right_low, right_top], axis=0),
        preferred_element_type=jnp.float32,
    )


def dot6(left, right):
    return jnp.dot(left, right, precision=HIGH, preferred_element_type=jnp.float32)


def block_inverse(block):
    size = block.shape[0]
    low, high = NOISE_MIN * 0.97, (size + 1.0) * 1.01
    eye = (
        lax.broadcasted_iota(jnp.int32, block.shape, 0)
        == lax.broadcasted_iota(jnp.int32, block.shape, 1)
    ).astype(jnp.float32)
    first = 2.0 / (low + high)
    gap = 1.0 - first * low
    scale = 2.0 / (2.0 - gap * gap)
    guess = (2.0 * first * scale) * eye - (first * first * scale) * block
    gap = gap * gap / (2.0 - gap * gap)
    while gap > 1e-3:
        scale = 2.0 / (2.0 - gap * gap)
        rest = 2.0 * eye - dot3(block, guess)
        guess = scale * dot3(guess, rest)
        gap = gap * gap / (2.0 - gap * gap)
    for _ in range(2):
        guess = guess + dot3(guess, eye - dot6(block, guess))
    return guess


def inverse_kernel(step, matrix_ref, out_ref):
    size = matrix_ref.shape[0]
    out_ref[...] = matrix_ref[...]
    for start in range(0, size, step):
        here = slice(start, start + step)
        pivot = block_inverse(out_ref[here, here])
        column = out_ref[:, here]
        row = dot6(pivot, out_ref[here, :])
        for low in range(0, size, step):
            if low != start:
                part = slice(low, low + step)
                out_ref[part, :] = out_ref[part, :] - dot6(column[part], row)
                out_ref[part, here] = -dot6(column[part], pivot)
        out_ref[here, :] = row
        out_ref[here, here] = pivot


def spd_inverse(matrix):
    size = matrix.shape[0]
    step = math.gcd(size, 128)
    return pl.pallas_call(
        functools.partial(inverse_kernel, step),
        out_shape=jax.ShapeDtypeStruct(matrix.shape, jnp.float32),
        in_specs=[VMEM],
        out_specs=VMEM,
        compiler_params=pltpu.CompilerParams(vmem_limit_bytes=32 * 1024 * 1024),
    )(matrix)


def sum_kernel(axes, left_ref, right_ref, out_ref, mine, *rest):
    slots, (send_sem, recv_sem) = rest[: len(axes)], rest[len(axes) :]
    barrier = pltpu.get_barrier_semaphore()
    greeted = 0
    for axis in axes:
        count = lax.axis_size(axis)
        for hop in range(1, count):
            other = lax.rem(lax.axis_index(axis) + hop, count)
            pl.semaphore_signal(barrier, inc=1, device_id={axis: other}, device_id_type=MESH)
            greeted += 1
    mine[0] = jnp.sum(left_ref[...] * right_ref[...], axis=0, keepdims=True)
    pl.semaphore_wait(barrier, greeted)
    for stage, axis in enumerate(axes):
        count = lax.axis_size(axis)
        copies = []
        for hop in range(1, count):
            other = lax.rem(lax.axis_index(axis) + hop, count)
            copy = pltpu.make_async_remote_copy(
                src_ref=mine.at[stage],
                dst_ref=slots[stage].at[hop - 1],
                send_sem=send_sem.at[stage],
                recv_sem=recv_sem.at[stage],
                device_id={axis: other},
                device_id_type=MESH,
            )
            copy.start()
            copies.append(copy)
        if copies:
            whole = pltpu.make_async_copy(slots[stage], slots[stage], recv_sem.at[stage])
            whole.wait()
            mine[stage + 1] = mine[stage] + jnp.sum(slots[stage][...], axis=0)
            pltpu.make_async_copy(slots[stage], slots[stage], send_sem.at[stage]).wait()
        else:
            mine[stage + 1] = mine[stage]
    out_ref[...] = mine[len(axes)]


def total_dot(first, second):
    axes = ("gy", "gx")
    width = first.shape[1]
    return pl.pallas_call(
        functools.partial(sum_kernel, axes),
        out_shape=jax.ShapeDtypeStruct((1, width), jnp.float32),
        in_specs=[VMEM, VMEM],
        out_specs=VMEM,
        scratch_shapes=[pltpu.VMEM((len(axes) + 1, 1, width), jnp.float32)]
        + [pltpu.VMEM((max(lax.axis_size(a) - 1, 1), 1, width), jnp.float32) for a in axes]
        + [pltpu.SemaphoreType.DMA((len(axes),)), pltpu.SemaphoreType.DMA((len(axes),))],
        compiler_params=pltpu.CompilerParams(collective_id=0, has_side_effects=True),
    )(first, second)[0]


def shards(right_side, coords, noise, intersect):
    points = right_side.shape[2]
    rhs_count = right_side.shape[3]
    intersect_len = intersect.shape[2]
    ext_len = points + intersect_len
    own_pos = coords.reshape(2, points)
    own_noise = noise.reshape(points)
    point_info = jnp.concatenate([own_pos, own_noise[None, :]], axis=0)
    info_cols = window_values(point_info)
    positions = [
        [
            jnp.stack(
                [
                    info_cols[col_off][row_off, 0] + float(row_off - 1),
                    info_cols[col_off][row_off, 1] + float(col_off - 1),
                ]
            )
            for col_off in range(3)
        ]
        for row_off in range(3)
    ]
    intersect_ids = intersect.reshape(intersect_len)
    block_id = intersect_ids // points
    row_in = intersect_ids % points
    row_of = block_id // 3
    col_of = block_id % 3
    local_id = row_of * points + row_in
    picked_info = [
        jnp.take(
            jnp.transpose(info_cols[col_off], (1, 0, 2)).reshape(3, 3 * points), local_id, axis=1
        )
        for col_off in range(3)
    ]
    chosen = jnp.where(
        col_of[None, :] == 0,
        picked_info[0],
        jnp.where(col_of[None, :] == 1, picked_info[1], picked_info[2]),
    )
    ov_pos = jnp.stack(
        [chosen[0] + (row_of - 1).astype(jnp.float32), chosen[1] + (col_of - 1).astype(jnp.float32)]
    )
    ext_pos = jnp.concatenate([own_pos, ov_pos], axis=1)
    ext_noise = jnp.concatenate([own_noise, chosen[2]])
    local_matrix = kernel_block(ext_pos, ext_pos) + jnp.diag(ext_noise)
    inverse = spd_inverse(local_matrix)
    near_ids = window_index(intersect_ids)
    point_iota = jnp.arange(points, dtype=jnp.int32)[:, None]
    row_base = (2 - jnp.arange(3, dtype=jnp.int32))[:, None] * 3
    selectors = []
    for col_off in range(3):
        own_rows = near_ids[col_off] - (row_base + (2 - col_off)) * points
        selectors.append((point_iota == own_rows.reshape(1, 3 * intersect_len)).astype(jnp.float32))

    def borrowed_rows(residue):
        requested = [
            lax.dot_general(
                selectors[col_off],
                residue,
                (((0,), (0,)), ((), ())),
                precision=HIGH,
                preferred_element_type=jnp.float32,
            ).reshape(3, intersect_len, rhs_count)
            for col_off in range(3)
        ]
        combined = jnp.stack([requested[col_off][1] for col_off in range(3)])
        for step_by, row_off in ((-1, 0), (1, 2)):
            outgoing = jnp.stack([requested[col_off][row_off] for col_off in range(3)])
            combined = combined + shifted(outgoing, "gx", step_by)
        gathered = combined[1]
        for step_by, col_off in ((-1, 0), (1, 2)):
            gathered = gathered + passed_along(combined[col_off], "gy", step_by)
        return gathered

    def precondition(residue):
        gathered = borrowed_rows(residue)
        extended = jnp.concatenate([residue, gathered], axis=0)
        solved = jnp.dot(inverse, extended, precision=HIGH, preferred_element_type=jnp.float32)
        returned = window_values(solved[points:])
        result = solved[:points]
        for col_off in range(3):
            result = result + jnp.dot(
                selectors[col_off],
                returned[col_off].reshape(3 * intersect_len, rhs_count),
                precision=HIGH,
                preferred_element_type=jnp.float32,
            )
        return result

    noise_col = own_noise[:, None]
    residual = right_side.reshape(points, rhs_count)
    solution = jnp.zeros_like(residual)
    precond = precondition(residual)
    direction = precond
    inner_now = total_dot(residual, precond)
    for iteration in range(ITERS):
        columns = window_values(direction)
        accumulated = noise_col * direction
        for operate_row_off in range(3):
            for operate_col_off in range(3):
                accumulated = accumulated + jnp.dot(
                    kernel_block(own_pos, positions[operate_row_off][operate_col_off]),
                    columns[operate_col_off][operate_row_off],
                    precision=HIGH,
                    preferred_element_type=jnp.float32,
                )
        step_size = inner_now / total_dot(direction, accumulated)
        solution = solution + step_size * direction
        residual = residual - step_size * accumulated
        if iteration + 1 < ITERS:
            precond = precondition(residual)
            inner_next = total_dot(residual, precond)
            direction = precond + inner_next / inner_now * direction
            inner_now = inner_next
    return (solution.reshape(1, 1, points, rhs_count), residual.reshape(1, 1, points, rhs_count))


def solution(mesh):
    placed = (
        P("gx", "gy", None, None),
        P("gx", "gy", None, None),
        P("gx", "gy", None),
        P("gx", "gy", None),
    )
    return jax.shard_map(
        shards,
        mesh=mesh,
        in_specs=placed,
        out_specs=(P("gx", "gy", None, None), P("gx", "gy", None, None)),
        check_vma=False,
    )
```

```python
import functools
import math

import jax
import jax.numpy as jnp
from jax import lax
from jax.experimental import pallas as pl
from jax.experimental.pallas import tpu as pltpu
from jax.sharding import PartitionSpec as P

ITERS = 3


RANGE_LEN = 0.25
ROOT_THREE = math.sqrt(3.0)
HIGH = lax.Precision.HIGHEST


def shifted(value, axis, by):
    count = lax.axis_size(axis)
    return lax.ppermute(value, axis, [(i, (i + by) % count) for i in range(count)])


def passed_along(block, axis, distance):
    devices = range(lax.axis_size(axis))
    route = [(i - distance, i) for i in devices if i - distance in devices]
    return lax.ppermute(block, axis, route)


def kernel_block(rows_pos, cols_pos):
    delta_x = rows_pos[0][:, None] - cols_pos[0][None, :]
    delta_y = rows_pos[1][:, None] - cols_pos[1][None, :]
    distance = jnp.sqrt(delta_x * delta_x + delta_y * delta_y)
    scaled = ROOT_THREE / RANGE_LEN * distance
    clipped = jnp.minimum(distance, 1.0)
    taper_val = jnp.square(jnp.square(1.0 - clipped)) * (4.0 * clipped + 1.0)
    return (1.0 + scaled) * jnp.exp(-scaled) * taper_val


def window_values(values):
    beside = {}
    for step_by in (1, -1):
        beside[step_by] = shifted(values, "gx", step_by)
    column = jnp.stack([beside[1], values, beside[-1]])
    across = {}
    for step_by in (1, -1):
        across[step_by] = passed_along(column, "gy", step_by)
    return [across[1], column, across[-1]]


def window_index(values):
    beside = {}
    for step_by in (1, -1):
        beside[step_by] = shifted(values, "gx", step_by)
    column = jnp.stack([beside[1], values, beside[-1]])
    across = {}
    for step_by in (1, -1):
        across[step_by] = passed_along(column, "gy", step_by)
    return [across[1], column, across[-1]]


CHUNKS = 2
MESH = pl.DeviceIdType.MESH
NOISE_MIN = 0.25
VMEM = pl.BlockSpec(memory_space=pltpu.VMEM)


def split(value):
    top = value.astype(jnp.bfloat16)
    return top, (value - top.astype(jnp.float32)).astype(jnp.bfloat16)


def split_outside(value):
    top = lax.reduce_precision(value, exponent_bits=8, mantissa_bits=7)
    return top.astype(jnp.bfloat16), (value - top).astype(jnp.bfloat16)


def dot3(left, right):
    left_top, left_low = split(left)
    right_top, right_low = split(right)
    return jnp.dot(
        jnp.concatenate([left_top, left_top, left_low], axis=1),
        jnp.concatenate([right_top, right_low, right_top], axis=0),
        preferred_element_type=jnp.float32,
    )


def dot6(left, right):
    return jnp.dot(left, right, precision=HIGH, preferred_element_type=jnp.float32)


def block_inverse(block):
    size = block.shape[0]
    low, high = NOISE_MIN * 0.97, (size + 1.0) * 1.01
    eye = (
        lax.broadcasted_iota(jnp.int32, block.shape, 0)
        == lax.broadcasted_iota(jnp.int32, block.shape, 1)
    ).astype(jnp.float32)
    first = 2.0 / (low + high)
    gap = 1.0 - first * low
    scale = 2.0 / (2.0 - gap * gap)
    guess = (2.0 * first * scale) * eye - (first * first * scale) * block
    gap = gap * gap / (2.0 - gap * gap)
    while gap > 1e-3:
        scale = 2.0 / (2.0 - gap * gap)
        rest = 2.0 * eye - dot3(block, guess)
        guess = scale * dot3(guess, rest)
        gap = gap * gap / (2.0 - gap * gap)
    for _ in range(2):
        guess = guess + dot3(guess, eye - dot6(block, guess))
    return guess


def inverse_kernel(step, matrix_ref, out_ref):
    size = matrix_ref.shape[0]
    out_ref[...] = matrix_ref[...]
    for start in range(0, size, step):
        here = slice(start, start + step)
        pivot = block_inverse(out_ref[here, here])
        column = out_ref[:, here]
        row = dot6(pivot, out_ref[here, :])
        for low in range(0, size, step):
            if low != start:
                part = slice(low, low + step)
                out_ref[part, :] = out_ref[part, :] - dot6(column[part], row)
                out_ref[part, here] = -dot6(column[part], pivot)
        out_ref[here, :] = row
        out_ref[here, here] = pivot


def spd_inverse(matrix):
    size = matrix.shape[0]
    step = math.gcd(size, 128)
    return pl.pallas_call(
        functools.partial(inverse_kernel, step),
        out_shape=jax.ShapeDtypeStruct(matrix.shape, jnp.float32),
        in_specs=[VMEM],
        out_specs=VMEM,
        compiler_params=pltpu.CompilerParams(vmem_limit_bytes=32 * 1024 * 1024),
    )(matrix)


def columns_of(count):
    return () if count == 1 else (1,) if count == 2 else (-1, 1)


def opposite(col_off, count):
    return col_off if count == 2 else -col_off


def offsets_of(count):
    near = [(-1, 0), (1, 0)]
    for col_off in columns_of(count):
        near += [(0, col_off), (-1, col_off), (1, col_off)]
    return near


def cg_kernel(
    rhs_ref, top_ref, low_ref, inv_top_ref, inv_low_ref, pick_ref, put_ref,
    solution_ref, residual_ref,
    asked, got, tail, back, precond, window, direction, image, mine, slots_y, slots_x,
    send_sem, recv_sem,
):
    size_x, size_y = lax.axis_size("gx"), lax.axis_size("gy")
    my_x, my_y = lax.axis_index("gx"), lax.axis_index("gy")
    near = offsets_of(size_y)
    points = rhs_ref.shape[0]
    borrowed = tail.shape[0]
    half = points // CHUNKS

    def inside(col_off):
        if col_off == 0 or size_y == 2:
            return None
        return my_y > 0 if col_off < 0 else my_y < size_y - 1

    def guarded(condition, action):
        if condition is None:
            action()
        else:
            pl.when(condition)(action)

    def target(row_off, col_off):
        place = {}
        if row_off:
            place["gx"] = lax.rem(my_x + row_off + size_x, size_x)
        if col_off:
            place["gy"] = 1 - my_y if size_y == 2 else my_y + col_off
        return place

    counter = [0]

    class Move:
        def __init__(self, source, dest, row_off, col_off):
            index = counter[0]
            counter[0] += 1
            self.copy = pltpu.make_async_remote_copy(
                src_ref=source,
                dst_ref=dest,
                send_sem=send_sem.at[index],
                recv_sem=recv_sem.at[index],
                device_id=target(row_off, col_off),
                device_id_type=MESH,
            )
            self.out = inside(col_off)
            self.into = inside(-col_off)

        def start(self):
            guarded(self.out, self.copy.start)

        def sent(self):
            guarded(self.out, self.copy.wait_send)

        def landed(self):
            guarded(self.into, self.copy.wait_recv)

    def slot(row_off, col_off):
        return near.index((-row_off, opposite(col_off, size_y)))

    barrier = pltpu.get_barrier_semaphore()
    greeted = 0
    for axis, here, count in (("gx", my_x, size_x), ("gy", my_y, size_y)):
        for hop in range(1, count):
            pl.semaphore_signal(
                barrier, inc=1, device_id={axis: lax.rem(here + hop, count)}, device_id_type=MESH
            )
            greeted += 1
    for row_off, col_off in near:
        if row_off and col_off:

            def greet(row_off=row_off, col_off=col_off):
                pl.semaphore_signal(
                    barrier, inc=1, device_id=target(row_off, col_off), device_id_type=MESH
                )

            guarded(inside(col_off), greet)
            there = inside(col_off)
            greeted = greeted + (1 if there is None else jnp.where(there, 1, 0))

    for col_off in columns_of(size_y):
        there = inside(col_off)
        if there is not None:

            def clear(col_off=col_off):
                for index, (_, col) in enumerate(near):
                    if col == col_off:
                        for iteration in range(ITERS):
                            got[iteration, index] = jnp.zeros(tail.shape, jnp.float32)
                            back[iteration, index] = jnp.zeros(tail.shape, jnp.float32)
                            window[iteration, index] = jnp.zeros(rhs_ref.shape, jnp.float32)

            pl.when(jnp.logical_not(there))(clear)

    def exact_dot(ones, value):
        top, low = split(value)
        return jnp.dot(ones, top, preferred_element_type=jnp.float32) + jnp.dot(
            ones, low, preferred_element_type=jnp.float32
        )

    def dot_parts(left_top, left_low, right):
        right_top, right_low = split(right)
        return (
            jnp.dot(left_top, right_top, preferred_element_type=jnp.float32)
            + jnp.dot(left_top, right_low, preferred_element_type=jnp.float32)
            + jnp.dot(left_low, right_top, preferred_element_type=jnp.float32)
        )

    def window_part(block, value):
        cols = slice(block * points, (block + 1) * points)
        return dot_parts(top_ref[:, cols], low_ref[:, cols], value)

    def total(iteration):
        for stage, (axis, here, count, slots) in enumerate(
            (("gy", my_y, size_y, slots_y), ("gx", my_x, size_x, slots_x))
        ):
            index = counter[0]
            counter[0] += 1
            for hop in range(1, count):
                pltpu.make_async_remote_copy(
                    src_ref=mine.at[iteration, stage],
                    dst_ref=slots.at[iteration, hop - 1],
                    send_sem=send_sem.at[index],
                    recv_sem=recv_sem.at[index],
                    device_id={axis: lax.rem(here + hop, count)},
                    device_id_type=MESH,
                ).start()
            so_far = mine[iteration, stage]
            if count > 1:
                held = slots.at[iteration]
                pltpu.make_async_copy(held, held, recv_sem.at[index]).wait()
                so_far = so_far + jnp.sum(slots[iteration], axis=0)
                pltpu.make_async_copy(held, held, send_sem.at[index]).wait()
            mine[iteration, stage + 1] = so_far
        return mine[iteration, 2]

    residual_ref[...] = rhs_ref[...]
    wait_entry = [True]
    inner_old = denominator = None
    for iteration in range(ITERS):
        requests = exact_dot(pick_ref[...], residual_ref[...])
        for index in range(len(near)):
            asked[index] = requests[index * borrowed : (index + 1) * borrowed]
        if wait_entry[0]:
            pl.semaphore_wait(barrier, greeted)
            wait_entry[0] = False
        moves = [
            Move(asked.at[index], got.at[iteration, slot(*offset)], *offset)
            for index, offset in enumerate(near)
        ]
        for move in moves:
            move.start()
        solved = dot_parts(
            inv_top_ref[:, :points], inv_low_ref[:, :points], residual_ref[...]
        )
        for move in moves:
            move.landed()
        gathered = jnp.sum(got[iteration], axis=0)
        solved = solved + dot_parts(inv_top_ref[:, points:], inv_low_ref[:, points:], gathered)
        tail[...] = solved[points:]
        precond[...] = solved[:points]
        returns = [Move(tail, back.at[iteration, slot(*offset)], *offset) for offset in near]
        for move in returns:
            move.start()
        for move in moves:
            move.sent()
        for move in returns:
            move.landed()
        returned = back[iteration].reshape(len(near) * borrowed, tail.shape[1])
        precond[...] = precond[...] + exact_dot(put_ref[...], returned)
        for move in returns:
            move.sent()

        sides, relays = [], []
        for chunk in range(CHUNKS):
            rows = pl.ds(chunk * half, half)
            for col_off in columns_of(size_y):
                index = slot(0, col_off)
                sides.append(
                    Move(precond.at[rows], window.at[iteration, index, rows], 0, col_off)
                )
                sides[-1].start()
        beside = [
            Move(precond, window.at[iteration, slot(row_off, 0)], row_off, 0)
            for row_off in (-1, 1)
        ]
        for move in beside:
            move.start()
        result = window_part(len(near), precond[...])
        place = 0
        for chunk in range(CHUNKS):
            rows = pl.ds(chunk * half, half)
            for col_off in columns_of(size_y):
                sides[place].landed()
                place += 1
                source = near.index((0, opposite(col_off, size_y)))
                for row_off in (-1, 1):
                    index = near.index((-row_off, opposite(col_off, size_y)))
                    move = Move(
                        window.at[iteration, source, rows],
                        window.at[iteration, index, rows],
                        row_off,
                        0,
                    )
                    there = inside(-col_off)
                    move.out = move.into = there
                    relays.append(move)
                    move.start()
        for index, (row_off, col_off) in enumerate(near):
            if row_off == 0:
                result = result + window_part(index, window[iteration, index])
        for move in beside:
            move.landed()
        for index, (row_off, col_off) in enumerate(near):
            if row_off and col_off == 0:
                result = result + window_part(index, window[iteration, index])
        for move in relays:
            move.landed()
        for index, (row_off, col_off) in enumerate(near):
            if row_off and col_off:
                result = result + window_part(index, window[iteration, index])
        fresh = precond[...]
        mine[iteration, 0, 0:1] = jnp.sum(residual_ref[...] * fresh, axis=0, keepdims=True)
        mine[iteration, 0, 1:2] = jnp.sum(fresh * result, axis=0, keepdims=True)
        if iteration:
            mine[iteration, 0, 2:3] = jnp.sum(fresh * image[...], axis=0, keepdims=True)
        else:
            mine[iteration, 0, 2:3] = jnp.zeros((1, fresh.shape[1]), jnp.float32)
        sums = total(iteration)
        for move in sides + beside + relays:
            move.sent()
        inner, curved, mixed = sums[0:1], sums[1:2], sums[2:3]
        if iteration:
            ratio = inner / inner_old
            denominator = curved + ratio * (2.0 * mixed + ratio * denominator)
            direction[...] = fresh + ratio * direction[...]
            image[...] = result + ratio * image[...]
        else:
            denominator = curved
            direction[...] = fresh
            image[...] = result
        inner_old = inner
        step_size = inner / denominator
        moved = step_size * direction[...]
        solution_ref[...] = solution_ref[...] + moved if iteration else moved
        residual_ref[...] = residual_ref[...] - step_size * image[...]


def conjugate_gradients(right_side, window_matrix, inverse, pick):
    near = offsets_of(lax.axis_size("gy"))
    points, width = right_side.shape
    borrowed = inverse.shape[0] - points
    size_x, size_y = lax.axis_size("gx"), lax.axis_size("gy")
    sides = len(columns_of(size_y))
    moves = ITERS * (2 * len(near) + 2 + 3 * CHUNKS * sides + 2)
    out = jax.ShapeDtypeStruct(right_side.shape, jnp.float32)
    block = pltpu.VMEM((points, width), jnp.float32)
    small = (len(near), borrowed, width)
    return pl.pallas_call(
        cg_kernel,
        out_shape=(out, out),
        in_specs=[VMEM] * 7,
        out_specs=(VMEM, VMEM),
        scratch_shapes=[
            pltpu.VMEM(small, jnp.float32),
            pltpu.VMEM((ITERS,) + small, jnp.float32),
            pltpu.VMEM((borrowed, width), jnp.float32),
            pltpu.VMEM((ITERS,) + small, jnp.float32),
            block,
            pltpu.VMEM((ITERS, len(near), points, width), jnp.float32),
            block,
            block,
            pltpu.VMEM((ITERS, 3, 3, width), jnp.float32),
            pltpu.VMEM((ITERS, max(size_y - 1, 1), 3, width), jnp.float32),
            pltpu.VMEM((ITERS, max(size_x - 1, 1), 3, width), jnp.float32),
            pltpu.SemaphoreType.DMA((moves,)),
            pltpu.SemaphoreType.DMA((moves,)),
        ],
        compiler_params=pltpu.CompilerParams(
            collective_id=0, has_side_effects=True, vmem_limit_bytes=56 * 1024 * 1024
        ),
    )(right_side, *split_outside(window_matrix), *split_outside(inverse), pick, pick.T)


def shards(right_side, coords, noise, intersect):
    points = right_side.shape[2]
    rhs_count = right_side.shape[3]
    intersect_len = intersect.shape[2]
    ext_len = points + intersect_len
    own_pos = coords.reshape(2, points)
    own_noise = noise.reshape(points)
    point_info = jnp.concatenate([own_pos, own_noise[None, :]], axis=0)
    info_cols = window_values(point_info)
    intersect_ids = intersect.reshape(intersect_len)
    block_id = intersect_ids // points
    row_in = intersect_ids % points
    row_of = block_id // 3
    col_of = block_id % 3
    local_id = row_of * points + row_in
    picked_info = [
        jnp.take(
            jnp.transpose(info_cols[col_off], (1, 0, 2)).reshape(3, 3 * points), local_id, axis=1
        )
        for col_off in range(3)
    ]
    chosen = jnp.where(
        col_of[None, :] == 0,
        picked_info[0],
        jnp.where(col_of[None, :] == 1, picked_info[1], picked_info[2]),
    )
    ov_pos = jnp.stack(
        [chosen[0] + (row_of - 1).astype(jnp.float32), chosen[1] + (col_of - 1).astype(jnp.float32)]
    )
    ext_pos = jnp.concatenate([own_pos, ov_pos], axis=1)
    ext_noise = jnp.concatenate([own_noise, chosen[2]])
    local_matrix = kernel_block(ext_pos, ext_pos) + jnp.diag(ext_noise)
    inverse = spd_inverse(local_matrix)
    near_ids = window_index(intersect_ids)
    count = lax.axis_size("gy")
    point_iota = jnp.arange(points, dtype=jnp.int32)[None, :]
    blocks, picks = [], []
    for row_off, col_off in offsets_of(count) + [(0, 0)]:
        step = col_off
        info, ids = info_cols[col_off + 1][row_off + 1], near_ids[col_off + 1][row_off + 1]
        if col_off and count == 2:
            first = lax.axis_index("gy") == 0
            step = jnp.where(first, 1, -1)
            info = jnp.where(first, info, info_cols[0][row_off + 1])
            ids = jnp.where(first, ids, near_ids[0][row_off + 1])
        shift = jnp.asarray(step, jnp.float32)
        blocks.append(
            kernel_block(own_pos, jnp.stack([info[0] + float(row_off), info[1] + shift]))
        )
        if row_off or col_off:
            own_rows = ids - (3 * (1 - row_off) + (1 - step)) * points
            picks.append((own_rows[:, None] == point_iota).astype(jnp.bfloat16))
    blocks[-1] = blocks[-1] + jnp.diag(own_noise)
    answer, residual = conjugate_gradients(
        right_side.reshape(points, rhs_count),
        jnp.concatenate(blocks, axis=1),
        inverse,
        jnp.concatenate(picks, axis=0),
    )
    return (answer.reshape(1, 1, points, rhs_count), residual.reshape(1, 1, points, rhs_count))


def solution(mesh):
    placed = (
        P("gx", "gy", None, None),
        P("gx", "gy", None, None),
        P("gx", "gy", None),
        P("gx", "gy", None),
    )
    return jax.shard_map(
        shards,
        mesh=mesh,
        in_specs=placed,
        out_specs=(P("gx", "gy", None, None), P("gx", "gy", None, None)),
        check_vma=False,
    )
```

```python
import functools
import math

import jax
import jax.numpy as jnp
from jax import lax
from jax.experimental import pallas as pl
from jax.experimental.pallas import tpu as pltpu
from jax.sharding import PartitionSpec as P

ITERS = 3


RANGE_LEN = 0.25
ROOT_THREE = math.sqrt(3.0)
HIGH = lax.Precision.HIGHEST


def shifted(value, axis, by):
    count = lax.axis_size(axis)
    return lax.ppermute(value, axis, [(i, (i + by) % count) for i in range(count)])


def passed_along(block, axis, distance):
    devices = range(lax.axis_size(axis))
    route = [(i - distance, i) for i in devices if i - distance in devices]
    return lax.ppermute(block, axis, route)


def kernel_block(rows_pos, cols_pos):
    delta_x = rows_pos[0][:, None] - cols_pos[0][None, :]
    delta_y = rows_pos[1][:, None] - cols_pos[1][None, :]
    distance = jnp.sqrt(delta_x * delta_x + delta_y * delta_y)
    scaled = ROOT_THREE / RANGE_LEN * distance
    clipped = jnp.minimum(distance, 1.0)
    taper_val = jnp.square(jnp.square(1.0 - clipped)) * (4.0 * clipped + 1.0)
    return (1.0 + scaled) * jnp.exp(-scaled) * taper_val


def window_values(values):
    beside = {}
    for step_by in (1, -1):
        beside[step_by] = shifted(values, "gx", step_by)
    column = jnp.stack([beside[1], values, beside[-1]])
    across = {}
    for step_by in (1, -1):
        across[step_by] = passed_along(column, "gy", step_by)
    return [across[1], column, across[-1]]


CHUNKS = 4
MESH = pl.DeviceIdType.MESH
NOISE_MIN = 0.25
VMEM = pl.BlockSpec(memory_space=pltpu.VMEM)


def split(value):
    top = value.astype(jnp.bfloat16)
    return top, (value - top.astype(jnp.float32)).astype(jnp.bfloat16)


def dot3(left, right):
    left_top, left_low = split(left)
    right_top, right_low = split(right)
    return jnp.dot(
        jnp.concatenate([left_top, left_top, left_low], axis=1),
        jnp.concatenate([right_top, right_low, right_top], axis=0),
        preferred_element_type=jnp.float32,
    )


def dot6(left, right):
    return jnp.dot(left, right, precision=HIGH, preferred_element_type=jnp.float32)


def block_inverse(block):
    size = block.shape[0]
    low, high = NOISE_MIN * 0.97, (size + 1.0) * 1.01
    eye = (
        lax.broadcasted_iota(jnp.int32, block.shape, 0)
        == lax.broadcasted_iota(jnp.int32, block.shape, 1)
    ).astype(jnp.float32)
    first = 2.0 / (low + high)
    gap = 1.0 - first * low
    scale = 2.0 / (2.0 - gap * gap)
    guess = (2.0 * first * scale) * eye - (first * first * scale) * block
    gap = gap * gap / (2.0 - gap * gap)
    while gap > 1e-3:
        scale = 2.0 / (2.0 - gap * gap)
        rest = 2.0 * eye - dot3(block, guess)
        guess = scale * dot3(guess, rest)
        gap = gap * gap / (2.0 - gap * gap)
    for _ in range(2):
        guess = guess + dot3(guess, eye - dot6(block, guess))
    return guess


def invert(matrix_ref, out_ref):
    size = matrix_ref.shape[0]
    step = math.gcd(size, 128)
    out_ref[...] = matrix_ref[...]
    for start in range(0, size, step):
        here = slice(start, start + step)
        pivot = block_inverse(out_ref[here, here])
        column = out_ref[:, here]
        row = dot6(pivot, out_ref[here, :])
        for low in range(0, size, step):
            if low != start:
                part = slice(low, low + step)
                out_ref[part, :] = out_ref[part, :] - dot6(column[part], row)
                out_ref[part, here] = -dot6(column[part], pivot)
        out_ref[here, :] = row
        out_ref[here, here] = pivot


def columns_of(count):
    return () if count == 1 else (1,) if count == 2 else (-1, 1)


def opposite(col_off, count):
    return col_off if count == 2 else -col_off


def offsets_of(count):
    near = [(-1, 0), (1, 0)]
    for col_off in columns_of(count):
        near += [(0, col_off), (-1, col_off), (1, col_off)]
    return near


def cg_kernel(
    rhs_ref, window_ref, matrix_ref, pick_ref, put_ref,
    solution_ref, residual_ref,
    top_ref, low_ref, inverse, inv_top_ref, inv_low_ref, asked, got, tail, back, precond, window, direction, image, mine, slots_y, slots_x,
    send_sem, recv_sem,
):
    size_x, size_y = lax.axis_size("gx"), lax.axis_size("gy")
    my_x, my_y = lax.axis_index("gx"), lax.axis_index("gy")
    near = offsets_of(size_y)
    points = rhs_ref.shape[0]
    borrowed = tail.shape[0]
    half = points // CHUNKS

    def inside(col_off):
        if col_off == 0 or size_y == 2:
            return None
        return my_y > 0 if col_off < 0 else my_y < size_y - 1

    def guarded(condition, action):
        if condition is None:
            action()
        else:
            pl.when(condition)(action)

    def target(row_off, col_off):
        place = {}
        if row_off:
            place["gx"] = lax.rem(my_x + row_off + size_x, size_x)
        if col_off:
            place["gy"] = 1 - my_y if size_y == 2 else my_y + col_off
        return place

    counter = [0]

    class Move:
        def __init__(self, source, dest, row_off, col_off):
            index = counter[0]
            counter[0] += 1
            self.copy = pltpu.make_async_remote_copy(
                src_ref=source,
                dst_ref=dest,
                send_sem=send_sem.at[index],
                recv_sem=recv_sem.at[index],
                device_id=target(row_off, col_off),
                device_id_type=MESH,
            )
            self.out = inside(col_off)
            self.into = inside(-col_off)

        def start(self):
            guarded(self.out, self.copy.start)

        def sent(self):
            guarded(self.out, self.copy.wait_send)

        def landed(self):
            guarded(self.into, self.copy.wait_recv)

    def slot(row_off, col_off):
        return near.index((-row_off, opposite(col_off, size_y)))

    barrier = pltpu.get_barrier_semaphore()
    greeted = 0
    for axis, here, count in (("gx", my_x, size_x), ("gy", my_y, size_y)):
        for hop in range(1, count):
            pl.semaphore_signal(
                barrier, inc=1, device_id={axis: lax.rem(here + hop, count)}, device_id_type=MESH
            )
            greeted += 1
    for row_off, col_off in near:
        if row_off and col_off:

            def greet(row_off=row_off, col_off=col_off):
                pl.semaphore_signal(
                    barrier, inc=1, device_id=target(row_off, col_off), device_id_type=MESH
                )

            guarded(inside(col_off), greet)
            there = inside(col_off)
            greeted = greeted + (1 if there is None else jnp.where(there, 1, 0))

    for col_off in columns_of(size_y):
        there = inside(col_off)
        if there is not None:

            def clear(col_off=col_off):
                for index, (_, col) in enumerate(near):
                    if col == col_off:
                        for iteration in range(ITERS):
                            got[iteration, index] = jnp.zeros(tail.shape, jnp.float32)
                            back[iteration, index] = jnp.zeros(tail.shape, jnp.float32)
                            window[iteration, index] = jnp.zeros(rhs_ref.shape, jnp.float32)

            pl.when(jnp.logical_not(there))(clear)

    def exact_dot(ones, value):
        top, low = split(value)
        return jnp.dot(ones, top, preferred_element_type=jnp.float32) + jnp.dot(
            ones, low, preferred_element_type=jnp.float32
        )

    def dot_parts(left_top, left_low, right):
        right_top, right_low = split(right)
        return (
            jnp.dot(left_top, right_top, preferred_element_type=jnp.float32)
            + jnp.dot(left_top, right_low, preferred_element_type=jnp.float32)
            + jnp.dot(left_low, right_top, preferred_element_type=jnp.float32)
        )

    def window_part(block, value):
        cols = slice(block * points, (block + 1) * points)
        return dot_parts(top_ref[:, cols], low_ref[:, cols], value)

    def total(iteration):
        for stage, (axis, here, count, slots) in enumerate(
            (("gy", my_y, size_y, slots_y), ("gx", my_x, size_x, slots_x))
        ):
            index = counter[0]
            counter[0] += 1
            for hop in range(1, count):
                pltpu.make_async_remote_copy(
                    src_ref=mine.at[iteration, stage],
                    dst_ref=slots.at[iteration, hop - 1],
                    send_sem=send_sem.at[index],
                    recv_sem=recv_sem.at[index],
                    device_id={axis: lax.rem(here + hop, count)},
                    device_id_type=MESH,
                ).start()
            so_far = mine[iteration, stage]
            if count > 1:
                held = slots.at[iteration]
                pltpu.make_async_copy(held, held, recv_sem.at[index]).wait()
                so_far = so_far + jnp.sum(slots[iteration], axis=0)
                pltpu.make_async_copy(held, held, send_sem.at[index]).wait()
            mine[iteration, stage + 1] = so_far
        return mine[iteration, 2]

    residual_ref[...] = rhs_ref[...]
    wait_entry = [True]
    inner_old = denominator = None
    for iteration in range(ITERS):
        requests = exact_dot(pick_ref[...], residual_ref[...])
        for index in range(len(near)):
            asked[index] = requests[index * borrowed : (index + 1) * borrowed]
        if wait_entry[0]:
            pl.semaphore_wait(barrier, greeted)
            wait_entry[0] = False
        moves = [
            Move(asked.at[index], got.at[iteration, slot(*offset)], *offset)
            for index, offset in enumerate(near)
        ]
        for move in moves:
            move.start()
        if iteration == 0:
            invert(matrix_ref, inverse)
            inv_top_ref[...], inv_low_ref[...] = split(inverse[...])
            top_ref[...], low_ref[...] = split(window_ref[...])
        solved = dot_parts(
            inv_top_ref[:, :points], inv_low_ref[:, :points], residual_ref[...]
        )
        for move in moves:
            move.landed()
        gathered = jnp.sum(got[iteration], axis=0)
        solved = solved + dot_parts(inv_top_ref[:, points:], inv_low_ref[:, points:], gathered)
        tail[...] = solved[points:]
        precond[...] = solved[:points]
        returns = [Move(tail, back.at[iteration, slot(*offset)], *offset) for offset in near]
        for move in returns:
            move.start()
        for move in moves:
            move.sent()
        for move in returns:
            move.landed()
        returned = back[iteration].reshape(len(near) * borrowed, tail.shape[1])
        precond[...] = precond[...] + exact_dot(put_ref[...], returned)
        for move in returns:
            move.sent()

        sides, relays = [], []
        for chunk in range(CHUNKS):
            rows = pl.ds(chunk * half, half)
            for col_off in columns_of(size_y):
                index = slot(0, col_off)
                sides.append(
                    Move(precond.at[rows], window.at[iteration, index, rows], 0, col_off)
                )
                sides[-1].start()
        beside = [
            Move(precond, window.at[iteration, slot(row_off, 0)], row_off, 0)
            for row_off in (-1, 1)
        ]
        for move in beside:
            move.start()
        result = window_part(len(near), precond[...])
        place = 0
        for chunk in range(CHUNKS):
            rows = pl.ds(chunk * half, half)
            for col_off in columns_of(size_y):
                sides[place].landed()
                place += 1
                source = near.index((0, opposite(col_off, size_y)))
                for row_off in (-1, 1):
                    index = near.index((-row_off, opposite(col_off, size_y)))
                    move = Move(
                        window.at[iteration, source, rows],
                        window.at[iteration, index, rows],
                        row_off,
                        0,
                    )
                    there = inside(-col_off)
                    move.out = move.into = there
                    relays.append(move)
                    move.start()
        for index, (row_off, col_off) in enumerate(near):
            if row_off == 0:
                result = result + window_part(index, window[iteration, index])
        for move in beside:
            move.landed()
        for index, (row_off, col_off) in enumerate(near):
            if row_off and col_off == 0:
                result = result + window_part(index, window[iteration, index])
        for move in relays:
            move.landed()
        for index, (row_off, col_off) in enumerate(near):
            if row_off and col_off:
                result = result + window_part(index, window[iteration, index])
        fresh = precond[...]
        mine[iteration, 0, 0:1] = jnp.sum(residual_ref[...] * fresh, axis=0, keepdims=True)
        mine[iteration, 0, 1:2] = jnp.sum(fresh * result, axis=0, keepdims=True)
        if iteration:
            mine[iteration, 0, 2:3] = jnp.sum(fresh * image[...], axis=0, keepdims=True)
        else:
            mine[iteration, 0, 2:3] = jnp.zeros((1, fresh.shape[1]), jnp.float32)
        sums = total(iteration)
        for move in sides + beside + relays:
            move.sent()
        inner, curved, mixed = sums[0:1], sums[1:2], sums[2:3]
        if iteration:
            ratio = inner / inner_old
            denominator = curved + ratio * (2.0 * mixed + ratio * denominator)
            direction[...] = fresh + ratio * direction[...]
            image[...] = result + ratio * image[...]
        else:
            denominator = curved
            direction[...] = fresh
            image[...] = result
        inner_old = inner
        step_size = inner / denominator
        moved = step_size * direction[...]
        solution_ref[...] = solution_ref[...] + moved if iteration else moved
        residual_ref[...] = residual_ref[...] - step_size * image[...]


def conjugate_gradients(right_side, window_matrix, matrix, pick):
    near = offsets_of(lax.axis_size("gy"))
    points, width = right_side.shape
    borrowed = matrix.shape[0] - points
    size_x, size_y = lax.axis_size("gx"), lax.axis_size("gy")
    sides = len(columns_of(size_y))
    moves = ITERS * (2 * len(near) + 2 + 3 * CHUNKS * sides + 2)
    out = jax.ShapeDtypeStruct(right_side.shape, jnp.float32)
    block = pltpu.VMEM((points, width), jnp.float32)
    small = (len(near), borrowed, width)
    return pl.pallas_call(
        cg_kernel,
        out_shape=(out, out),
        in_specs=[VMEM] * 5,
        out_specs=(VMEM, VMEM),
        scratch_shapes=[
            pltpu.VMEM(window_matrix.shape, jnp.bfloat16),
            pltpu.VMEM(window_matrix.shape, jnp.bfloat16),
            pltpu.VMEM(matrix.shape, jnp.float32),
            pltpu.VMEM(matrix.shape, jnp.bfloat16),
            pltpu.VMEM(matrix.shape, jnp.bfloat16),
            pltpu.VMEM(small, jnp.float32),
            pltpu.VMEM((ITERS,) + small, jnp.float32),
            pltpu.VMEM((borrowed, width), jnp.float32),
            pltpu.VMEM((ITERS,) + small, jnp.float32),
            block,
            pltpu.VMEM((ITERS, len(near), points, width), jnp.float32),
            block,
            block,
            pltpu.VMEM((ITERS, 3, 3, width), jnp.float32),
            pltpu.VMEM((ITERS, max(size_y - 1, 1), 3, width), jnp.float32),
            pltpu.VMEM((ITERS, max(size_x - 1, 1), 3, width), jnp.float32),
            pltpu.SemaphoreType.DMA((moves,)),
            pltpu.SemaphoreType.DMA((moves,)),
        ],
        compiler_params=pltpu.CompilerParams(
            collective_id=0, has_side_effects=True, vmem_limit_bytes=56 * 1024 * 1024
        ),
    )(right_side, window_matrix, matrix, pick, pick.T)


def shards(right_side, coords, noise, intersect):
    points = right_side.shape[2]
    rhs_count = right_side.shape[3]
    intersect_len = intersect.shape[2]
    ext_len = points + intersect_len
    own_pos = coords.reshape(2, points)
    own_noise = noise.reshape(points)
    listed = jnp.pad(intersect.reshape(intersect_len), (0, points - intersect_len))
    point_info = jnp.concatenate(
        [own_pos, own_noise[None, :], listed.astype(jnp.float32)[None, :]], axis=0
    )
    info_cols = window_values(point_info)
    intersect_ids = intersect.reshape(intersect_len)
    block_id = intersect_ids // points
    row_in = intersect_ids % points
    row_of = block_id // 3
    col_of = block_id % 3
    local_id = row_of * points + row_in
    picked_info = [
        jnp.take(
            jnp.transpose(info_cols[col_off], (1, 0, 2)).reshape(4, 3 * points), local_id, axis=1
        )
        for col_off in range(3)
    ]
    chosen = jnp.where(
        col_of[None, :] == 0,
        picked_info[0],
        jnp.where(col_of[None, :] == 1, picked_info[1], picked_info[2]),
    )
    ov_pos = jnp.stack(
        [chosen[0] + (row_of - 1).astype(jnp.float32), chosen[1] + (col_of - 1).astype(jnp.float32)]
    )
    ext_pos = jnp.concatenate([own_pos, ov_pos], axis=1)
    ext_noise = jnp.concatenate([own_noise, chosen[2]])
    local_matrix = kernel_block(ext_pos, ext_pos) + jnp.diag(ext_noise)
    count = lax.axis_size("gy")
    point_iota = jnp.arange(points, dtype=jnp.int32)[None, :]
    blocks, picks = [], []
    for row_off, col_off in offsets_of(count) + [(0, 0)]:
        step = col_off
        info = info_cols[col_off + 1][row_off + 1]
        if col_off and count == 2:
            first = lax.axis_index("gy") == 0
            step = jnp.where(first, 1, -1)
            info = jnp.where(first, info, info_cols[0][row_off + 1])
        shift = jnp.asarray(step, jnp.float32)
        blocks.append(
            kernel_block(own_pos, jnp.stack([info[0] + float(row_off), info[1] + shift]))
        )
        if row_off or col_off:
            ids = info[3, :intersect_len].astype(jnp.int32)
            own_rows = ids - (3 * (1 - row_off) + (1 - step)) * points
            picks.append((own_rows[:, None] == point_iota).astype(jnp.bfloat16))
    blocks[-1] = blocks[-1] + jnp.diag(own_noise)
    answer, residual = conjugate_gradients(
        right_side.reshape(points, rhs_count),
        jnp.concatenate(blocks, axis=1),
        local_matrix,
        jnp.concatenate(picks, axis=0),
    )
    return (answer.reshape(1, 1, points, rhs_count), residual.reshape(1, 1, points, rhs_count))


def solution(mesh):
    placed = (
        P("gx", "gy", None, None),
        P("gx", "gy", None, None),
        P("gx", "gy", None),
        P("gx", "gy", None),
    )
    return jax.shard_map(
        shards,
        mesh=mesh,
        in_specs=placed,
        out_specs=(P("gx", "gy", None, None), P("gx", "gy", None, None)),
        check_vma=False,
    )
```
